32 devices in a mesh: seq: 8 (over z, x), head: 4 (over y, core).
Axes of the slice: x: 2, y: 2, z: 4, core: 2. Of those that a mesh axis runs over, the one named last changes fastest.
Arguments:
- queries: bfloat16 [4096, 4096], P('seq', 'head'), may hold values from -6 to 6
- keys: bfloat16 [4096, 4096], P('seq', 'head'), may hold values from -6 to 6
- values: bfloat16 [4096, 4096], P('seq', 'head'), may hold values from -6 to 6
- med_weight: float32 [2, 32, 4], P(None, 'head'), may hold values from -3 to 3
- coarse_weight: float32 [2, 32, 64], P(None, 'head'), may hold values from -0.75 to 0.75
- out_weight: bfloat16 [4096, 4096], P('head'), may hold values from -0.09375 to 0.09375
Outputs:
- mixed: bfloat16 [4096, 4096], P('seq', 'head')
The draws below stay inside these ranges and needn't reach their ends.
All inputs are finite; a program needn't handle non-finite values.
Results may differ from the reference program's by a relative error of at most 0.013.
Values may be sent and summed in bfloat16 or wider, within the bound.
A program may use at most 128 MiB of HBM per device.

```python
import math
import jax
import jax.numpy as jnp
from jax import lax

D = 4096
HEADS = 32
HEAD_DIM = 128
TOK_DEV = 512
WIN = 512
MED = 4
COARSE = 64
TOKENS = 4096
N_SEQ = 8
N_HEAD = 4


def draw_queries(key, part):
    noise_key = jax.random.fold_in(key, 11)
    draws_bulk = jnp.clip(jax.random.normal(noise_key, (TOKENS, HEADS * HEAD_DIM), jnp.float32), -6.0, 6.0)
    return draws_bulk.astype(jnp.bfloat16)


def draw_keys(key, part):
    noise_key = jax.random.fold_in(key, 23)
    draws_bulk = jnp.clip(jax.random.normal(noise_key, (TOKENS, HEADS * HEAD_DIM), jnp.float32), -6.0, 6.0)
    return draws_bulk.astype(jnp.bfloat16)


def block_levels(stream_key, dims, cuts, smallest, top_value):
    def one(dim, shards_of):
        steps = jax.random.uniform(jax.random.fold_in(jax.random.fold_in(stream_key, 6), dim), (shards_of,), jnp.float32, smallest / len(cuts), top_value / len(cuts))
        return jnp.repeat(jnp.exp(steps), dims[dim] // shards_of).reshape((-1,) + (1,) * (len(dims) - dim - 1))

    gain = one(*cuts[0])
    for cut in cuts[1:]:
        gain = gain * one(*cut)
    return gain


def normal_values(stream_key, extent, spread, reach, pieces=(), kind=jnp.bfloat16):
    values = spread * jax.random.normal(stream_key, extent, jnp.float32)
    if pieces:
        values = values * block_levels(stream_key, extent, pieces, -0.22, 0.18)
    return jnp.clip(values, -reach, reach).astype(kind)


def setup_inputs(seed: int = 0) -> dict:
    arg_keys = jax.random.split(jax.random.key(seed), 7)
    queries = draw_queries(jax.random.fold_in(arg_keys[6], 71), 0)
    keys = draw_keys(jax.random.fold_in(arg_keys[6], 71), 0)
    values = normal_values(arg_keys[2], (TOKENS, HEADS * HEAD_DIM), 1.0, 6.0, ((0, 8), (1, 4)))
    med_weight = normal_values(arg_keys[3], (2, HEADS, MED), MED ** -0.5, 3.0, ((1, 4),), jnp.float32)
    coarse_weight = normal_values(arg_keys[4], (2, HEADS, COARSE), COARSE ** -0.5, 0.75, ((1, 4),), jnp.float32)
    out_weight = normal_values(arg_keys[5], (HEADS * HEAD_DIM, D), (HEADS * HEAD_DIM) ** -0.5, 0.09375, ((0, 4),))
    return dict(queries=queries, keys=keys, values=values, med_weight=med_weight, coarse_weight=coarse_weight, out_weight=out_weight)


def summarize(tensor, weight, ratio):
    groups = tensor.shape[0] // ratio
    grouped = tensor.reshape(groups, ratio, tensor.shape[1], tensor.shape[2]).astype(jnp.float32)
    return jnp.einsum('jrhd,hr->jhd', grouped, weight.astype(jnp.float32)).astype(jnp.bfloat16)

def reference(queries, keys, values, med_weight, coarse_weight, out_weight):
    head_width = HEAD_DIM
    query3 = queries.reshape(TOKENS, HEADS, head_width)
    key3 = keys.reshape(TOKENS, HEADS, head_width)
    value3 = values.reshape(TOKENS, HEADS, head_width)
    med_keys = summarize(key3, med_weight[0], MED)
    med_values = summarize(value3, med_weight[1], MED)
    coarse_keys = summarize(key3, coarse_weight[0], COARSE)
    coarse_values = summarize(value3, coarse_weight[1], COARSE)
    per_med = TOK_DEV // MED
    per_coarse = TOK_DEV // COARSE
    group_width = HEADS * head_width // N_HEAD
    score_scale = 1.0 / math.sqrt(head_width)
    coarse_owner = jnp.arange(TOKENS // COARSE, dtype=jnp.int32) // per_coarse

    def one_block(position):
        first = position * TOK_DEV
        query_blk = lax.dynamic_slice_in_dim(query3, first, TOK_DEV, 0)
        edge_first = jnp.maximum(first - WIN, 0).astype(jnp.int32)
        key_list = [lax.dynamic_slice_in_dim(key3, first, TOK_DEV, 0), lax.dynamic_slice_in_dim(key3, edge_first, WIN, 0)]
        value_list = [lax.dynamic_slice_in_dim(value3, first, TOK_DEV, 0), lax.dynamic_slice_in_dim(value3, edge_first, WIN, 0)]
        place_list = [jnp.arange(TOK_DEV, dtype=jnp.int32), jnp.full((WIN,), -1, jnp.int32)]
        usable_list = [jnp.ones((TOK_DEV,), bool), jnp.broadcast_to(position >= 1, (WIN,))]
        for distance in (2, 3, 4):
            med_first = (jnp.maximum(position - distance, 0) * per_med).astype(jnp.int32)
            key_list.append(lax.dynamic_slice_in_dim(med_keys, med_first, per_med, 0))
            value_list.append(lax.dynamic_slice_in_dim(med_values, med_first, per_med, 0))
            place_list.append(jnp.full((per_med,), -1, jnp.int32))
            usable_list.append(jnp.broadcast_to(position >= distance, (per_med,)))
        key_list.append(coarse_keys)
        value_list.append(coarse_values)
        place_list.append(jnp.full((TOKENS // COARSE,), -1, jnp.int32))
        usable_list.append(coarse_owner <= position - 1)
        key_all = jnp.concatenate(key_list, 0)
        value_all = jnp.concatenate(value_list, 0)
        key_place = jnp.concatenate(place_list, 0)
        usable = jnp.concatenate(usable_list, 0)
        query_place = jnp.arange(TOK_DEV, dtype=jnp.int32)
        allowed = (key_place[None, :] <= query_place[:, None]) & usable[None, :]
        scores = jnp.einsum('qhd,khd->hqk', query_blk.astype(jnp.float32), key_all.astype(jnp.float32)) * score_scale
        scores = jnp.where(allowed[None], scores, -jnp.inf)
        row_peak = lax.optimization_barrier(jnp.max(scores, axis=-1, keepdims=True))
        exp_scores = jnp.exp(scores - row_peak)
        row_total = lax.optimization_barrier(jnp.sum(exp_scores, axis=-1))
        rounded = lax.optimization_barrier(exp_scores.astype(jnp.bfloat16)).astype(jnp.float32)
        weighted = jnp.einsum('hqk,khd->hqd', rounded, value_all.astype(jnp.float32))
        attention = (weighted / row_total[..., None]).astype(jnp.bfloat16)
        attention = attention.transpose(1, 0, 2).reshape(TOK_DEV, HEADS * head_width)
        mixed = jnp.zeros((TOK_DEV, D), jnp.float32)
        for member in range(N_HEAD):
            partial_sum = jnp.dot(attention[:, member * group_width:(member + 1) * group_width], out_weight[member * group_width:(member + 1) * group_width], preferred_element_type=jnp.float32)
            mixed = mixed + lax.optimization_barrier(partial_sum.astype(jnp.bfloat16)).astype(jnp.float32)
        return mixed.astype(jnp.bfloat16)
    blocks = lax.map(one_block, jnp.arange(N_SEQ, dtype=jnp.int32))
    return blocks.reshape(TOKENS, D)
```

```python
import functools
import math

import jax
import jax.numpy as jnp
from jax import lax
from jax.experimental import pallas as pl
from jax.experimental.pallas import tpu as pltpu
from jax.sharding import PartitionSpec as P

MESH = pl.DeviceIdType.MESH
F32 = jnp.float32
BF16 = jnp.bfloat16
LOG2E = math.log2(math.e)


def mm(a, b):
    return jnp.dot(a, b, preferred_element_type=F32)


def mm_nt(a, b):
    return lax.dot_general(a, b, (((1,), (1,)), ((), ())), preferred_element_type=F32)


def split(w):
    hi = w.astype(BF16)
    return hi, (w - hi.astype(F32)).astype(BF16)


def kernel(
    n_seq, n_head, q_hbm, k_hbm, v_hbm, wm_hbm, wc_hbm, w_hbm, out_hbm,
    q_v, k_v, v_v, wm_v, wc_v, pat, w_v, vt, q_in, oe_out, le_out, oe_in, le_in,
    med_own, med_in, c_own, c_in, ck, cvt, o_loc, m_loc, l_loc, attn, attn_in,
    far_out, far_in, acc, out_v,
    ld_sem, w_sem, wx_ss, wx_rs, q_ss, q_rs, oe_ss, oe_rs, le_ss, le_rs, med_ss, med_rs,
    c_ss, c_rs, at_ss, at_rs, far_ss, far_rs, out_sem,
):
    tok, feat = q_v.shape
    med, _, heads = wm_v.shape
    coarse = wc_v.shape[2]
    dim = feat // heads
    row = oe_in.shape[3]
    chunks = tok // row
    wide = 2 * row
    n_med = tok // med
    n_coarse = tok // coarse
    width = out_v.shape[1]
    tile = far_out.shape[4]
    tiles = width // tile
    scale = LOG2E / math.sqrt(dim)
    pos = lax.axis_index("seq")
    hd = lax.axis_index("head")
    groups = n_head // 2
    grp = hd // 2
    core = lax.rem(hd, 2)
    mate = grp * 2 + (1 - core)

    def remote(src, dst, ss, rs, **dev):
        return pltpu.make_async_remote_copy(
            src_ref=src, dst_ref=dst, send_sem=ss, recv_sem=rs,
            device_id=dev, device_id_type=MESH,
        )

    def hs(h):
        return pl.ds(pl.multiple_of(h * dim, dim), dim)

    loads = [
        pltpu.make_async_copy(s, d, ld_sem.at[n])
        for n, (s, d) in enumerate(
            ((wm_hbm, wm_v), (wc_hbm, wc_v), (k_hbm, k_v), (v_hbm, v_v), (q_hbm, q_v))
        )
    ]
    for ld in loads:
        ld.start()

    barrier = pltpu.get_barrier_semaphore()

    @pl.loop(1, n_seq)
    def _(d):
        pl.semaphore_signal(
            barrier, inc=1, device_id={"seq": lax.rem(pos + d, n_seq)}, device_id_type=MESH
        )

    @pl.loop(1, n_head)
    def _(d):
        pl.semaphore_signal(
            barrier, inc=1, device_id={"head": lax.rem(hd + d, n_head)}, device_id_type=MESH
        )

    @pl.loop(0, n_seq)
    def _(o):
        @pl.when(o >= pos)
        def _():
            c_in[o] = jnp.zeros(c_in.shape[1:], BF16)

    for slot in range(2):
        @pl.when(pos < 2 * slot + 2)
        def _():
            med_in[slot] = jnp.zeros(med_in.shape[1:], BF16)

    @pl.when(pos == 0)
    def _():
        oe_in[...] = jnp.zeros_like(oe_in)
        le_in[...] = jnp.full_like(le_in, -jnp.inf)

    loads[0].wait()
    loads[1].wait()
    for n, (src, size) in enumerate(((wm_v, med), (wc_v, coarse))):
        lane = lax.broadcasted_iota(jnp.int32, (size, row), 1)
        pick = lax.rem(lane, size) == lax.broadcasted_iota(jnp.int32, (size, row), 0)
        pick = jnp.where(pick, 1.0, 0.0).astype(BF16)
        for t in range(2):
            hi, lo = split(src[t] if n else src[:, t, :].T)
            pat[n, 0, t] = mm(hi, pick)
            pat[n, 1, t] = mm(lo, pick)

    pl.semaphore_wait(barrier, n_seq - 1 + n_head - 1)

    def rows(i):
        return pl.ds(i * row, row)

    def q_copy(i):
        return remote(
            q_hbm.at[rows(i)], q_in.at[rows(i)], q_ss.at[i], q_rs.at[i],
            seq=jnp.maximum(pos - 1, 0),
        )

    def oe_copy(i):
        return remote(
            oe_out.at[i], oe_in.at[i], oe_ss.at[i], oe_rs.at[i],
            seq=jnp.minimum(pos + 1, n_seq - 1),
        )

    def le_copy(i):
        return remote(
            le_out.at[i], le_in.at[i], le_ss.at[i], le_rs.at[i],
            seq=jnp.minimum(pos + 1, n_seq - 1),
        )

    def med_copy(slot):
        src = med_own if slot == 0 else med_in.at[0]
        return remote(
            src, med_in.at[slot], med_ss.at[slot], med_rs.at[slot],
            seq=jnp.minimum(pos + 2, n_seq - 1),
        )

    def c_copy(to):
        return remote(c_own, c_in.at[pos], c_ss.at[to], c_rs.at[pos], seq=to)

    def cols(g, side):
        return pl.ds(pl.multiple_of((g * 2 + side) * width, width), width)

    def w_load(g):
        return pltpu.make_async_copy(w_hbm.at[:, cols(g, core)], w_v.at[0, g], w_sem.at[g])

    def w_copy(g):
        return remote(
            w_hbm.at[:, cols(g, 1 - core)], w_v.at[1, g], wx_ss.at[g], wx_rs.at[g], head=mate
        )

    def at_copy(i):
        return remote(attn.at[rows(i)], attn_in.at[rows(i)], at_ss.at[i], at_rs.at[i], head=mate)

    def far_copy(i, o, j):
        return remote(
            far_out.at[i, o - 1, j], far_in.at[i, o - 1, j],
            far_ss.at[i, o - 1, j], far_rs.at[i, o - 1, j],
            head=lax.rem(grp + o, groups) * 2 + core,
        )

    def out_copy(i):
        return pltpu.make_async_copy(out_v.at[rows(i)], out_hbm.at[rows(i)], out_sem.at[i])

    has_prev = pos >= 1
    has_next = pos < n_seq - 1

    @pl.when(has_prev)
    def _():
        for i in range(chunks):
            q_copy(i).start()

    loads[2].wait()
    loads[3].wait()

    per = row // med
    sel = (lax.broadcasted_iota(jnp.int32, (per, row), 1) // med) == (
        lax.broadcasted_iota(jnp.int32, (per, row), 0)
    )
    c_row = lax.broadcasted_iota(jnp.int32, (2 * n_coarse, tok), 0)
    c_col = lax.broadcasted_iota(jnp.int32, (2 * n_coarse, tok), 1) // coarse

    @pl.loop(0, heads)
    def _(h):
        vt[h] = v_v[:, hs(h)].T
        pooled = []
        totals = []
        for t, src in enumerate((k_v, v_v)):
            one = pl.ds(h, 1)
            left = jnp.concatenate(
                [jnp.where(sel, pat[0, part, t, one, :], 0.0) for part in range(2)], axis=0
            ).astype(BF16)
            blocks = []
            for b in range(chunks):
                r = mm(left, src[rows(b), hs(h)])
                blocks.append((r[:per] + r[per:]).astype(BF16))
            pooled.append(jnp.concatenate(blocks, axis=0))
            hi, lo = (
                jnp.concatenate([pat[1, part, t, one, :]] * chunks, axis=1) for part in range(2)
            )
            left = jnp.where(c_col == c_row, hi, 0.0)
            left = jnp.where(c_col + n_coarse == c_row, lo, left).astype(BF16)
            r = mm(left, src[:, hs(h)])
            totals.append(r[:n_coarse] + r[n_coarse:])
        med_own[0, h] = pooled[0]
        med_own[1, h] = pooled[1].T
        c_own[h] = jnp.concatenate(totals, axis=0).astype(BF16)

    @pl.when(pos + 2 < n_seq)
    def _():
        med_copy(0).start()

    for g in range(groups):
        w_copy(g).start()
        w_load(g).start()

    @pl.loop(0, n_seq)
    def _(to):
        @pl.when(to > pos)
        def _():
            c_copy(to).start()

    loads[4].wait()

    def keep(i, h, o, m, total):
        for n in range(2):
            at = slice(n * row, (n + 1) * row)
            o_loc[2 * i + n, h] = o[:, at]
            m_loc[2 * i + n, pl.ds(h, 1), :] = m[:, at]
            l_loc[2 * i + n, pl.ds(h, 1), :] = total[:, at]

    def softmax_parts(parts, m, total, o):
        for s, vals in parts:
            p = jnp.exp2((s - m) * scale)
            total = total + jnp.sum(p, axis=0, keepdims=True)
            o = o + mm(vals, p.astype(BF16))
        return total, o

    def peak(parts):
        return functools.reduce(
            jnp.maximum, [jnp.max(s, axis=0, keepdims=True) for s, _ in parts]
        )

    def own(i):
        first = i * wide

        @pl.loop(0, heads)
        def _(h):
            q = q_v[pl.ds(first, wide), hs(h)]
            parts = []
            if first:
                s = mm_nt(k_v[pl.ds(0, first), hs(h)], q)
                parts.append((s, vt[h, :, pl.ds(0, first)]))
            s = mm_nt(k_v[pl.ds(first, wide), hs(h)], q)
            key_at = lax.broadcasted_iota(jnp.int32, (wide, wide), 0)
            query_at = lax.broadcasted_iota(jnp.int32, (wide, wide), 1)
            s = jnp.where(key_at <= query_at, s, -jnp.inf)
            parts.append((s, vt[h, :, pl.ds(first, wide)]))
            m = peak(parts)
            total, o = softmax_parts(parts, m, 0.0, 0.0)
            keep(i, h, o, m, total)

    def edge(i):
        @pl.when(has_next)
        def _():
            @pl.loop(0, heads)
            def _(h):
                q = q_in[pl.ds(i * wide, wide), hs(h)]
                s = mm_nt(k_v[:, hs(h)], q)
                s2 = jnp.where(pos >= 2, mm_nt(med_in[0, 0, h], q), -jnp.inf)
                parts = [(s, vt[h]), (s2, med_in[0, 1, h])]
                m = peak(parts)
                total, o = softmax_parts(parts, m, 0.0, 0.0)
                o = (o / total).astype(BF16)
                lse = m * scale + jnp.log2(total)
                for n in range(2):
                    at = slice(n * row, (n + 1) * row)
                    oe_out[2 * i + n, h] = o[:, at]
                    le_out[2 * i + n, pl.ds(h, 1), :] = lse[:, at]

    def await_queries(i):
        @pl.when(has_next)
        def _():
            q_copy(2 * i).wait_recv()
            q_copy(2 * i + 1).wait_recv()

    def send_edge(i):
        @pl.when(has_next)
        def _():
            for n in range(2):
                le_copy(2 * i + n).start()
                oe_copy(2 * i + n).start()

    def remote_parts(i):
        @pl.loop(0, heads)
        def _(h):
            q = q_v[pl.ds(i * wide, wide), hs(h)]
            parts = []
            for slot in range(2):
                s = mm_nt(med_in[slot, 0, h], q)
                parts.append((jnp.where(pos >= 2 * slot + 2, s, -jnp.inf), med_in[slot, 1, h]))
            s = mm_nt(ck[h], q)
            owner = lax.broadcasted_iota(jnp.int32, s.shape, 0) // n_coarse
            parts.append((jnp.where(owner < pos, s, -jnp.inf), cvt[h]))
            both = (2 * i, 2 * i + 1)
            old = jnp.concatenate([m_loc[c, pl.ds(h, 1), :] for c in both], axis=1)
            total = jnp.concatenate([l_loc[c, pl.ds(h, 1), :] for c in both], axis=1)
            o = jnp.concatenate([o_loc[c, h] for c in both], axis=1)
            m = jnp.maximum(old, peak(parts))
            a = jnp.exp2((old - m) * scale)
            total, o = softmax_parts(parts, m, total * a, o * a)
            keep(i, h, o, m, total)

    def combine(i):
        @pl.when(has_prev)
        def _():
            le_copy(i).wait_recv()
            oe_copy(i).wait_recv()

        mine = m_loc[i] * scale
        lse = le_in[i]
        top = jnp.maximum(mine, lse)
        a = jnp.exp2(mine - top)
        e = jnp.exp2(lse - top)
        inv = 1.0 / (l_loc[i] * a + e)
        a = a * inv
        e = e * inv
        for h in range(heads):
            o = o_loc[i, h] * a[h:h + 1] + oe_in[i, h].astype(F32) * e[h:h + 1]
            attn[rows(i), h * dim:(h + 1) * dim] = o.astype(BF16).T
        at_copy(i).start()

    def mix(i):
        waited = False
        for o in list(range(1, groups)) + [0]:
            g = lax.rem(grp + o, groups)

            for j in range(tiles):
                at = pl.ds(j * tile, tile)
                acc[i, :, at] = mm(attn[rows(i)], w_v[0, g, :, at])
            if not waited:
                at_copy(i).wait_recv()
                waited = True
            for j in range(tiles):
                at = pl.ds(j * tile, tile)
                value = acc[i, :, at] + mm(attn_in[rows(i)], w_v[1, g, :, at])
                if o:
                    far_out[i, o - 1, j] = value.astype(BF16)
                    far_copy(i, o, j).start()
                else:
                    acc[i, :, at] = value

    def final(i):
        for j in range(tiles):
            at = pl.ds(j * tile, tile)
            total = acc[i, :, at]
            for o in range(1, groups):
                far_copy(i, o, j).wait_recv()
                total = total + far_in[i, o - 1, j].astype(F32)
            out_v[rows(i), at] = total.astype(BF16)
        out_copy(i).start()

    for i in range(chunks // 2):
        own(i)

    @pl.when(pos >= 2)
    def _():
        med_copy(0).wait_recv()

        @pl.when(pos + 2 < n_seq)
        def _():
            med_copy(1).start()

    halves = chunks // 2
    await_queries(0)
    for i in range(halves):
        edge(i)
        if i + 1 < halves:
            await_queries(i + 1)
        if i + 2 >= halves:
            for n in range(i if i + 2 > halves else 0, i + 1):
                send_edge(n)

    @pl.loop(0, n_seq)
    def _(o):
        @pl.when(o < pos)
        def _():
            remote(c_own, c_in.at[o], c_ss.at[o], c_rs.at[o], seq=o).wait_recv()

    @pl.loop(0, heads)
    def _(h):
        got = c_in[:, h].astype(F32)
        ck[h] = got[:, :n_coarse].reshape(n_seq * n_coarse, dim).astype(BF16)
        cvt[h] = got[:, n_coarse:].reshape(n_seq * n_coarse, dim).T.astype(BF16)

    @pl.when(pos >= 4)
    def _():
        med_copy(1).wait_recv()

    for i in range(chunks // 2):
        remote_parts(i)

    for g in range(groups):
        w_load(g).wait()
        w_copy(g).wait_recv()

    for i in range(chunks):
        combine(i)
        mix(i)
        if i:
            final(i - 1)
    final(chunks - 1)

    @pl.when(has_prev)
    def _():
        for i in range(chunks):
            q_copy(i).wait_send()

    @pl.when(has_next)
    def _():
        for i in range(chunks):
            le_copy(i).wait_send()
            oe_copy(i).wait_send()

    @pl.when(pos + 2 < n_seq)
    def _():
        med_copy(0).wait_send()

    @pl.when((pos >= 2) & (pos + 2 < n_seq))
    def _():
        med_copy(1).wait_send()

    @pl.loop(0, n_seq)
    def _(to):
        @pl.when(to > pos)
        def _():
            c_copy(to).wait_send()

    for g in range(groups):
        w_copy(g).wait_send()
    for i in range(chunks):
        at_copy(i).wait_send()
        for o in range(1, groups):
            for j in range(tiles):
                far_copy(i, o, j).wait_send()
    for i in range(chunks):
        out_copy(i).wait()


def body(n_seq, n_head, queries, keys, values, med_weight, coarse_weight, out_weight):
    tok, feat = queries.shape
    heads, med = med_weight.shape[1:]
    dim = feat // heads
    row = dim
    chunks = tok // row
    width = out_weight.shape[1] // n_head
    groups = n_head // 2
    far = max(groups - 1, 1)
    tile = math.gcd(width, 4 * dim)
    tiles = width // tile
    n_med = tok // med
    n_coarse = tok // coarse_weight.shape[2]
    dma = pltpu.SemaphoreType.DMA
    hbm = pl.BlockSpec(memory_space=pl.ANY)
    V = pltpu.VMEM
    scratch = [
        V((tok, feat), BF16), V((tok, feat), BF16), V((tok, feat), BF16),
        V((med, 2, heads), F32), V(coarse_weight.shape, F32),
        V((2, 2, 2, heads, row), F32),
        V((2, groups, feat, width), BF16),
        V((heads, dim, tok), BF16),
        V((tok, feat), BF16),
        V((chunks, heads, dim, row), BF16),
        V((chunks, heads, row), F32),
        V((chunks, heads, dim, row), BF16),
        V((chunks, heads, row), F32),
        V((2, heads, n_med, dim), BF16),
        V((2, 2, heads, n_med, dim), BF16),
        V((heads, 2 * n_coarse, dim), BF16),
        V((n_seq, heads, 2 * n_coarse, dim), BF16),
        V((heads, n_seq * n_coarse, dim), BF16),
        V((heads, dim, n_seq * n_coarse), BF16),
        V((chunks, heads, dim, row), F32),
        V((chunks, heads, row), F32),
        V((chunks, heads, row), F32),
        V((tok, feat), BF16),
        V((tok, feat), BF16),
        V((chunks, far, tiles, row, tile), BF16),
        V((chunks, far, tiles, row, tile), BF16),
        V((chunks, row, width), F32),
        V((tok, width), BF16),
        dma((5,)), dma((groups,)), dma((groups,)), dma((groups,)),
        dma((chunks,)), dma((chunks,)),
        dma((chunks,)), dma((chunks,)),
        dma((chunks,)), dma((chunks,)),
        dma((2,)), dma((2,)),
        dma((n_seq,)), dma((n_seq,)),
        dma((chunks,)), dma((chunks,)),
        dma((chunks, far, tiles)), dma((chunks, far, tiles)),
        dma((chunks,)),
    ]
    return pl.pallas_call(
        functools.partial(kernel, n_seq, n_head),
        out_shape=jax.ShapeDtypeStruct((tok, width), BF16),
        in_specs=[hbm] * 6,
        out_specs=hbm,
        scratch_shapes=scratch,
        compiler_params=pltpu.CompilerParams(
            collective_id=0, has_side_effects=True, vmem_limit_bytes=60 * 1024 * 1024
        ),
    )(queries, keys, values, med_weight.transpose(2, 0, 1), coarse_weight, out_weight)


def solution(mesh):
    placed = (
        P("seq", "head"),
        P("seq", "head"),
        P("seq", "head"),
        P(None, "head", None),
        P(None, "head", None),
        P("head", None),
    )
    return jax.shard_map(
        functools.partial(body, mesh.shape["seq"], mesh.shape["head"]),
        mesh=mesh, in_specs=placed, out_specs=P("seq", "head"), check_vma=False,
    )
```

```python
import functools
import math

import jax
import jax.numpy as jnp
from jax import lax
from jax.experimental import pallas as pl
from jax.experimental.pallas import tpu as pltpu
from jax.sharding import PartitionSpec as P

MESH = pl.DeviceIdType.MESH
F32 = jnp.float32
BF16 = jnp.bfloat16
LOG2E = math.log2(math.e)


def mm(a, b):
    return jnp.dot(a, b, preferred_element_type=F32)


def mm_nt(a, b):
    return lax.dot_general(a, b, (((1,), (1,)), ((), ())), preferred_element_type=F32)


def split(w):
    hi = w.astype(BF16)
    return hi, (w - hi.astype(F32)).astype(BF16)


def row_pieces(tok, row):
    cuts = list(range(0, tok, row)) + [tok - row // 2, tok]
    return list(zip(cuts[:-1], cuts[1:]))


def kernel(
    n_seq, n_head, q_hbm, k_hbm, v_hbm, wm_hbm, wc_hbm, w_hbm, out_ref,
    q_v, k_v, v_v, wm_v, wc_v, pat, w_v, vt, q_in, oe_out, le_out, oe_in, le_in,
    med_own, med_in, c_own, c_in, ck, cvt, o_loc, m_loc, l_loc, a_loc, e_col, o_rows,
    attn, attn_in, far_out, far_in, acc,
    ld_sem, w_sem, wx_ss, wx_rs, q_ss, q_rs, oe_ss, oe_rs, le_ss, le_rs, med_ss, med_rs,
    c_ss, c_rs, at_ss, at_rs, far_ss, far_rs,
):
    tok, feat = q_v.shape
    _, med, heads = wm_v.shape
    coarse = wc_v.shape[2]
    dim = feat // heads
    row = dim
    chunks = tok // row
    wide = 2 * row
    halves = tok // wide
    pieces = row_pieces(tok, row)
    n_med = tok // med
    n_coarse = tok // coarse
    width = out_ref.shape[1]
    tile = far_out.shape[3]
    tiles = width // tile
    scale = LOG2E / math.sqrt(dim)
    pos = lax.axis_index("seq")
    hd = lax.axis_index("head")
    groups = n_head // 2
    grp = hd // 2
    core = lax.rem(hd, 2)
    mate = grp * 2 + (1 - core)

    def remote(src, dst, ss, rs, **dev):
        return pltpu.make_async_remote_copy(
            src_ref=src, dst_ref=dst, send_sem=ss, recv_sem=rs,
            device_id=dev, device_id_type=MESH,
        )

    def hs(h):
        return pl.ds(pl.multiple_of(h * dim, dim), dim)

    loads = [
        pltpu.make_async_copy(s, d, ld_sem.at[n])
        for n, (s, d) in enumerate(
            ((wm_hbm, wm_v), (wc_hbm, wc_v), (k_hbm, k_v), (v_hbm, v_v), (q_hbm, q_v))
        )
    ]
    for ld in loads:
        ld.start()

    barrier = pltpu.get_barrier_semaphore()

    @pl.loop(1, n_seq)
    def _(d):
        pl.semaphore_signal(
            barrier, inc=1, device_id={"seq": lax.rem(pos + d, n_seq)}, device_id_type=MESH
        )

    @pl.loop(1, n_head)
    def _(d):
        pl.semaphore_signal(
            barrier, inc=1, device_id={"head": lax.rem(hd + d, n_head)}, device_id_type=MESH
        )

    @pl.loop(0, n_seq)
    def _(o):
        @pl.when(o >= pos)
        def _():
            c_in[o] = jnp.zeros(c_in.shape[1:], BF16)

    for slot in range(2):
        @pl.when(pos < 2 * slot + 2)
        def _():
            med_in[slot] = jnp.zeros(med_in.shape[1:], BF16)

    @pl.when(pos == 0)
    def _():
        oe_in[...] = jnp.zeros_like(oe_in)
        le_in[...] = jnp.full_like(le_in, -jnp.inf)

    loads[0].wait()
    loads[1].wait()
    for n, (src, size) in enumerate(((wm_v, med), (wc_v, coarse))):
        lane = lax.broadcasted_iota(jnp.int32, (size, row), 1)
        pick = lax.rem(lane, size) == lax.broadcasted_iota(jnp.int32, (size, row), 0)
        pick = jnp.where(pick, 1.0, 0.0).astype(BF16)
        for t in range(2):
            hi, lo = split(src[t] if n else src[t].T)
            pat[n, 0, t] = mm(hi, pick)
            pat[n, 1, t] = mm(lo, pick)

    pl.semaphore_wait(barrier, n_seq - 1 + n_head - 1)

    def rows(i):
        return pl.ds(i * row, row)

    def q_copy(i):
        return remote(
            q_hbm.at[rows(i)], q_in.at[rows(i)], q_ss.at[i], q_rs.at[i],
            seq=jnp.maximum(pos - 1, 0),
        )

    def part(c):
        return pl.ds(pieces[c][0], pieces[c][1] - pieces[c][0])

    def oe_copy(c):
        return remote(
            oe_out.at[part(c)], oe_in.at[part(c)], oe_ss.at[c], oe_rs.at[c],
            seq=jnp.minimum(pos + 1, n_seq - 1),
        )

    def le_copy(i):
        return remote(
            le_out.at[i], le_in.at[i], le_ss.at[i], le_rs.at[i],
            seq=jnp.minimum(pos + 1, n_seq - 1),
        )

    def med_copy(slot, t):
        src = med_own if slot == 0 else med_in.at[0]
        return remote(
            src.at[t], med_in.at[slot, t], med_ss.at[slot, t], med_rs.at[slot, t],
            seq=jnp.minimum(pos + 2, n_seq - 1),
        )

    def c_copy(to):
        return remote(c_own, c_in.at[pos], c_ss.at[to], c_rs.at[pos], seq=to)

    def cols(g, side):
        return pl.ds(pl.multiple_of((g * 2 + side) * width, width), width)

    def w_load(g):
        return pltpu.make_async_copy(w_hbm.at[:, cols(g, core)], w_v.at[0, g], w_sem.at[g])

    def w_copy(g):
        return remote(
            w_hbm.at[:, cols(g, 1 - core)], w_v.at[1, g], wx_ss.at[g], wx_rs.at[g], head=mate
        )

    def at_copy(c):
        return remote(attn.at[part(c)], attn_in.at[part(c)], at_ss.at[c], at_rs.at[c], head=mate)

    def far_copy(c, o, j):
        return remote(
            far_out.at[o - 1, j, part(c)], far_in.at[o - 1, j, part(c)],
            far_ss.at[c, o - 1, j], far_rs.at[c, o - 1, j],
            head=lax.rem(grp + o, groups) * 2 + core,
        )

    has_prev = pos >= 1
    has_next = pos < n_seq - 1

    @pl.when(has_prev)
    def _():
        for i in range(chunks):
            q_copy(i).start()

    for g in range(groups):
        w_copy(g).start()
        w_load(g).start()
    loads[2].wait()
    loads[3].wait()

    per = row // med
    sel = (lax.broadcasted_iota(jnp.int32, (per, row), 1) // med) == (
        lax.broadcasted_iota(jnp.int32, (per, row), 0)
    )
    c_row = lax.broadcasted_iota(jnp.int32, (2 * n_coarse, tok), 0)
    c_col = lax.broadcasted_iota(jnp.int32, (2 * n_coarse, tok), 1) // coarse

    for t, src in enumerate((k_v, v_v)):
        @pl.loop(0, heads)
        def _(h):
            one = pl.ds(h, 1)
            left = jnp.concatenate(
                [jnp.where(sel, pat[0, n, t, one, :], 0.0) for n in range(2)], axis=0
            ).astype(BF16)
            blocks = []
            for b in range(chunks):
                r = mm(left, src[rows(b), hs(h)])
                blocks.append((r[:per] + r[per:]).astype(BF16))
            pooled = jnp.concatenate(blocks, axis=0)
            med_own[t, h] = pooled.T if t else pooled

        @pl.when(pos + 2 < n_seq)
        def _():
            med_copy(0, t).start()

    @pl.loop(0, heads)
    def _(h):
        vt[h] = v_v[:, hs(h)].T
        totals = []
        for t, src in enumerate((k_v, v_v)):
            hi, lo = (
                jnp.concatenate([pat[1, n, t, pl.ds(h, 1), :]] * chunks, axis=1)
                for n in range(2)
            )
            left = jnp.where(c_col == c_row, hi, 0.0)
            left = jnp.where(c_col + n_coarse == c_row, lo, left).astype(BF16)
            r = mm(left, src[:, hs(h)])
            totals.append(r[:n_coarse] + r[n_coarse:])
        c_own[h] = jnp.concatenate(totals, axis=0).astype(BF16)

    @pl.loop(0, n_seq)
    def _(to):
        @pl.when(to > pos)
        def _():
            c_copy(to).start()

    loads[4].wait()

    def keep(i, h, o, m, total):
        o_loc[i, h] = o
        m_loc[i, pl.ds(h, 1), :] = m
        l_loc[i, pl.ds(h, 1), :] = total

    def softmax_parts(parts, m, total, o):
        for s, vals in parts:
            p = jnp.exp2((s - m) * scale)
            total = total + jnp.sum(p, axis=0, keepdims=True)
            o = o + mm(vals, p.astype(BF16))
        return total, o

    def peak(parts):
        return functools.reduce(
            jnp.maximum, [jnp.max(s, axis=0, keepdims=True) for s, _ in parts]
        )

    def own(i):
        first = i * wide

        @pl.loop(0, heads, unroll=2)
        def _(h):
            q = q_v[pl.ds(first, wide), hs(h)]
            parts = []
            if first:
                s = mm_nt(k_v[pl.ds(0, first), hs(h)], q)
                parts.append((s, vt[h, :, pl.ds(0, first)]))
            s = mm_nt(k_v[pl.ds(first, wide), hs(h)], q)
            key_at = lax.broadcasted_iota(jnp.int32, (wide, wide), 0)
            query_at = lax.broadcasted_iota(jnp.int32, (wide, wide), 1)
            s = jnp.where(key_at <= query_at, s, -jnp.inf)
            parts.append((s, vt[h, :, pl.ds(first, wide)]))
            m = peak(parts)
            total, o = softmax_parts(parts, m, 0.0, 0.0)
            keep(i, h, o, m, total)

    def edge(i):
        @pl.when(has_next)
        def _():
            @pl.loop(0, heads, unroll=2)
            def _(h):
                q = q_in[pl.ds(i * wide, wide), hs(h)]
                s = mm_nt(k_v[:, hs(h)], q)
                s2 = jnp.where(pos >= 2, mm_nt(med_in[0, 0, h], q), -jnp.inf)
                parts = [(s, vt[h]), (s2, med_in[0, 1, h])]
                m = peak(parts)
                total, o = softmax_parts(parts, m, 0.0, 0.0)
                oe_out[pl.ds(i * wide, wide), hs(h)] = (o / total).astype(BF16).T
                le_out[i, pl.ds(h, 1), :] = m * scale + jnp.log2(total)

            le_copy(i).start()

    def await_queries(i):
        @pl.when(has_next)
        def _():
            q_copy(2 * i).wait_recv()
            q_copy(2 * i + 1).wait_recv()

    def send_edge(i):
        @pl.when(has_next)
        def _():
            for c, (first, _) in enumerate(pieces):
                if first // wide == i:
                    oe_copy(c).start()

    def remote_parts(i):
        @pl.loop(0, heads, unroll=2)
        def _(h):
            q = q_v[pl.ds(i * wide, wide), hs(h)]
            parts = []
            for slot in range(2):
                s = mm_nt(med_in[slot, 0, h], q)
                parts.append((jnp.where(pos >= 2 * slot + 2, s, -jnp.inf), med_in[slot, 1, h]))
            s = mm_nt(ck[h], q)
            owner = lax.broadcasted_iota(jnp.int32, s.shape, 0) // n_coarse
            parts.append((jnp.where(owner < pos, s, -jnp.inf), cvt[h]))
            old = m_loc[i, pl.ds(h, 1), :]
            total = l_loc[i, pl.ds(h, 1), :]
            o = o_loc[i, h]
            m = jnp.maximum(old, peak(parts))
            a = jnp.exp2((old - m) * scale)
            total, o = softmax_parts(parts, m, total * a, o * a)
            keep(i, h, o, m, total)

    def prepare(i):
        @pl.when(has_prev)
        def _():
            le_copy(i).wait_recv()

        mine = m_loc[i] * scale
        lse = le_in[i]
        top = jnp.maximum(mine, lse)
        a = jnp.exp2(mine - top)
        e = jnp.exp2(lse - top)
        inv = 1.0 / (l_loc[i] * a + e)
        a_loc[...] = a * inv
        e_col[pl.ds(i * wide, wide), :] = (e * inv).T

        @pl.loop(0, heads)
        def _(h):
            o_rows[pl.ds(i * wide, wide), hs(h)] = (o_loc[i, h] * a_loc[pl.ds(h, 1), :]).T

    def combine(c):
        @pl.when(has_prev)
        def _():
            oe_copy(c).wait_recv()

        for h in range(heads):
            at = slice(h * dim, (h + 1) * dim)
            o = o_rows[part(c), at] + oe_in[part(c), at].astype(F32) * e_col[part(c), h:h + 1]
            attn[part(c), at] = o.astype(BF16)
        at_copy(c).start()

    def mix(c):
        waited = False
        for o in list(range(1, groups)) + [0]:
            g = lax.rem(grp + o, groups)
            for j in range(tiles):
                at = pl.ds(j * tile, tile)
                acc[part(c), at] = mm(attn[part(c)], w_v[0, g, :, at])
            if not waited:
                at_copy(c).wait_recv()
                waited = True
            for j in range(tiles):
                at = pl.ds(j * tile, tile)
                value = acc[part(c), at] + mm(attn_in[part(c)], w_v[1, g, :, at])
                if o:
                    far_out[o - 1, j, part(c)] = value.astype(BF16)
                    far_copy(c, o, j).start()
                else:
                    acc[part(c), at] = value

    def final(c):
        for j in range(tiles):
            at = pl.ds(j * tile, tile)
            total = acc[part(c), at]
            for o in range(1, groups):
                far_copy(c, o, j).wait_recv()
                total = total + far_in[o - 1, j, part(c)].astype(F32)
            out_ref[part(c), at] = total.astype(BF16)

    def pass_on(t):
        @pl.when(pos >= 2)
        def _():
            med_copy(0, t).wait_recv()

            @pl.when(pos + 2 < n_seq)
            def _():
                med_copy(1, t).start()

    for i in range(halves):
        own(i)
        if i < 2:
            pass_on(i)

    await_queries(0)
    for i in range(halves):
        edge(i)
        if i + 1 < halves:
            await_queries(i + 1)
        send_edge(i)

    @pl.loop(0, n_seq)
    def _(o):
        @pl.when(o < pos)
        def _():
            remote(c_own, c_in.at[o], c_ss.at[o], c_rs.at[o], seq=o).wait_recv()

    @pl.loop(0, heads)
    def _(h):
        got = c_in[:, h].astype(F32)
        ck[h] = got[:, :n_coarse].reshape(n_seq * n_coarse, dim).astype(BF16)
        cvt[h] = got[:, n_coarse:].reshape(n_seq * n_coarse, dim).T.astype(BF16)

    @pl.when(pos >= 4)
    def _():
        med_copy(1, 0).wait_recv()
        med_copy(1, 1).wait_recv()

    for g in range(groups):
        w_load(g).wait()
        w_copy(g).wait_recv()

    for c, (first, _) in enumerate(pieces):
        if first % wide == 0:
            @pl.when(has_prev)
            def _():
                remote_parts(first // wide)

            prepare(first // wide)
        combine(c)
        mix(c)
    for c in range(len(pieces)):
        final(c)

    @pl.when(has_prev)
    def _():
        for i in range(chunks):
            q_copy(i).wait_send()

    @pl.when(has_next)
    def _():
        for i in range(halves):
            le_copy(i).wait_send()
        for c in range(len(pieces)):
            oe_copy(c).wait_send()

    @pl.when(pos + 2 < n_seq)
    def _():
        med_copy(0, 0).wait_send()
        med_copy(0, 1).wait_send()

    @pl.when((pos >= 2) & (pos + 2 < n_seq))
    def _():
        med_copy(1, 0).wait_send()
        med_copy(1, 1).wait_send()

    @pl.loop(0, n_seq)
    def _(to):
        @pl.when(to > pos)
        def _():
            c_copy(to).wait_send()

    for g in range(groups):
        w_copy(g).wait_send()
    for c in range(len(pieces)):
        at_copy(c).wait_send()
        for o in range(1, groups):
            for j in range(tiles):
                far_copy(c, o, j).wait_send()


def body(n_seq, n_head, queries, keys, values, med_weight, coarse_weight, out_weight):
    tok, feat = queries.shape
    heads, med = med_weight.shape[1:]
    dim = feat // heads
    row = dim
    chunks = tok // row
    wide = 2 * row
    halves = tok // wide
    pieces = len(row_pieces(tok, row))
    width = out_weight.shape[1] // n_head
    groups = n_head // 2
    far = max(groups - 1, 1)
    tile = math.gcd(width, 4 * dim)
    tiles = width // tile
    n_med = tok // med
    n_coarse = tok // coarse_weight.shape[2]
    dma = pltpu.SemaphoreType.DMA
    hbm = pl.BlockSpec(memory_space=pl.ANY)
    V = pltpu.VMEM
    scratch = [
        V((tok, feat), BF16), V((tok, feat), BF16), V((tok, feat), BF16),
        V((2, med, heads), F32), V(coarse_weight.shape, F32),
        V((2, 2, 2, heads, row), F32),
        V((2, groups, feat, width), BF16),
        V((heads, dim, tok), BF16),
        V((tok, feat), BF16),
        V((tok, feat), BF16),
        V((halves, heads, wide), F32),
        V((tok, feat), BF16),
        V((halves, heads, wide), F32),
        V((2, heads, n_med, dim), BF16),
        V((2, 2, heads, n_med, dim), BF16),
        V((heads, 2 * n_coarse, dim), BF16),
        V((n_seq, heads, 2 * n_coarse, dim), BF16),
        V((heads, n_seq * n_coarse, dim), BF16),
        V((heads, dim, n_seq * n_coarse), BF16),
        V((halves, heads, dim, wide), F32),
        V((halves, heads, wide), F32),
        V((halves, heads, wide), F32),
        V((heads, wide), F32),
        V((tok, heads), F32),
        V((tok, feat), F32),
        V((tok, feat), BF16),
        V((tok, feat), BF16),
        V((far, tiles, tok, tile), BF16),
        V((far, tiles, tok, tile), BF16),
        V((tok, width), F32),
        dma((5,)), dma((groups,)), dma((groups,)), dma((groups,)),
        dma((chunks,)), dma((chunks,)),
        dma((pieces,)), dma((pieces,)),
        dma((halves,)), dma((halves,)),
        dma((2, 2)), dma((2, 2)),
        dma((n_seq,)), dma((n_seq,)),
        dma((pieces,)), dma((pieces,)),
        dma((pieces, far, tiles)), dma((pieces, far, tiles)),
    ]
    return pl.pallas_call(
        functools.partial(kernel, n_seq, n_head),
        out_shape=jax.ShapeDtypeStruct((tok, width), BF16),
        in_specs=[hbm] * 6,
        out_specs=pl.BlockSpec(memory_space=pltpu.VMEM),
        scratch_shapes=scratch,
        compiler_params=pltpu.CompilerParams(
            collective_id=0, has_side_effects=True, vmem_limit_bytes=48 * 1024 * 1024
        ),
    )(*(
        pltpu.with_memory_space_constraint(x, pltpu.HBM)
        for x in (
            queries, keys, values, med_weight.transpose(0, 2, 1), coarse_weight, out_weight
        )
    ))


def solution(mesh):
    placed = (
        P("seq", "head"),
        P("seq", "head"),
        P("seq", "head"),
        P(None, "head", None),
        P(None, "head", None),
        P("head", None),
    )
    return jax.shard_map(
        functools.partial(body, mesh.shape["seq"], mesh.shape["head"]),
        mesh=mesh, in_specs=placed, out_specs=P("seq", "head"), check_vma=False,
    )
```

```python
import functools
import math

import jax
import jax.numpy as jnp
from jax import lax
from jax.experimental import pallas as pl
from jax.experimental.pallas import tpu as pltpu
from jax.sharding import PartitionSpec as P

MESH = pl.DeviceIdType.MESH
F32 = jnp.float32
BF16 = jnp.bfloat16
LOG2E = math.log2(math.e)


def mm(a, b):
    return jnp.dot(a, b, preferred_element_type=F32)


def mm_nt(a, b):
    return lax.dot_general(a, b, (((1,), (1,)), ((), ())), preferred_element_type=F32)


def split(w):
    hi = w.astype(BF16)
    return hi, (w - hi.astype(F32)).astype(BF16)


def row_pieces(tok, row):
    cuts = list(range(0, tok, row)) + [tok - row // 2, tok]
    return list(zip(cuts[:-1], cuts[1:]))


def kernel(
    n_seq, n_head, q_hbm, k_hbm, v_hbm, wm_hbm, wc_hbm, w_hbm, out_ref,
    q_v, k_v, v_v, wm_v, wc_v, pat, w_v, vt, q_in, oe_out, le_out, oe_in, le_in,
    med_own, med_in, c_in, ck, cvt, o_loc, m_loc, l_loc, a_loc, e_col, o_rows,
    attn, attn_in, far_out, far_in, acc,
    ld_sem, w_sem, wx_ss, wx_rs, q_ss, q_rs, oe_ss, oe_rs, le_ss, le_rs, med_ss, med_rs,
    c_ss, c_rs, at_ss, at_rs, far_ss, far_rs,
):
    tok, feat = q_v.shape
    _, med, heads = wm_v.shape
    coarse = wc_v.shape[2]
    dim = feat // heads
    row = dim
    chunks = tok // row
    wide = 2 * row
    halves = tok // wide
    pieces = row_pieces(tok, row)
    n_med = tok // med
    n_coarse = tok // coarse
    width = out_ref.shape[1]
    tile = far_out.shape[3]
    tiles = width // tile
    scale = LOG2E / math.sqrt(dim)
    pos = lax.axis_index("seq")
    hd = lax.axis_index("head")
    groups = n_head // 2
    grp = hd // 2
    core = lax.rem(hd, 2)
    mate = grp * 2 + (1 - core)

    def remote(src, dst, ss, rs, **dev):
        return pltpu.make_async_remote_copy(
            src_ref=src, dst_ref=dst, send_sem=ss, recv_sem=rs,
            device_id=dev, device_id_type=MESH,
        )

    def hs(h):
        return pl.ds(pl.multiple_of(h * dim, dim), dim)

    loads = [
        pltpu.make_async_copy(s, d, ld_sem.at[n])
        for n, (s, d) in enumerate(
            ((wm_hbm, wm_v), (wc_hbm, wc_v), (k_hbm, k_v), (v_hbm, v_v), (q_hbm, q_v))
        )
    ]
    for ld in loads[:4]:
        ld.start()

    barrier = pltpu.get_barrier_semaphore()

    near_by = [(d, pos + d) for d in (-2, -1, 1, 2)]
    others = n_head - 1
    for d, to in near_by:
        there = to >= 0 if d < 0 else to < n_seq
        others = others + jnp.where(there, 1, 0)

        @pl.when(there)
        def _():
            pl.semaphore_signal(barrier, inc=1, device_id={"seq": to}, device_id_type=MESH)

    @pl.loop(1, n_head)
    def _(d):
        pl.semaphore_signal(
            barrier, inc=1, device_id={"head": lax.rem(hd + d, n_head)}, device_id_type=MESH
        )

    @pl.loop(0, n_seq)
    def _(o):
        @pl.when(o > pos)
        def _():
            c_in[o] = jnp.zeros(c_in.shape[1:], BF16)

    for slot in range(2):
        @pl.when(pos < 2 * slot + 2)
        def _():
            med_in[slot] = jnp.zeros(med_in.shape[1:], BF16)

    @pl.when(pos == 0)
    def _():
        oe_in[...] = jnp.zeros_like(oe_in)
        le_in[...] = jnp.full_like(le_in, -jnp.inf)

    loads[0].wait()
    loads[1].wait()
    for n, (src, size) in enumerate(((wm_v, med), (wc_v, coarse))):
        lane = lax.broadcasted_iota(jnp.int32, (size, row), 1)
        pick = lax.rem(lane, size) == lax.broadcasted_iota(jnp.int32, (size, row), 0)
        pick = jnp.where(pick, 1.0, 0.0).astype(BF16)
        for t in range(2):
            hi, lo = split(src[t] if n else src[t].T)
            pat[n, 0, t] = mm(hi, pick)
            pat[n, 1, t] = mm(lo, pick)

    def rows(i):
        return pl.ds(i * row, row)

    per = row // med
    sel = (lax.broadcasted_iota(jnp.int32, (per, row), 1) // med) == (
        lax.broadcasted_iota(jnp.int32, (per, row), 0)
    )
    loads[2].wait()
    loads[3].wait()

    @pl.when(pos + 2 < n_seq)
    def _():
        for t, src in enumerate((k_v, v_v)):
            @pl.loop(0, heads, unroll=2)
            def _(h):
                one = pl.ds(h, 1)
                left = jnp.concatenate(
                    [jnp.where(sel, pat[0, n, t, one, :], 0.0) for n in range(2)], axis=0
                ).astype(BF16)
                blocks = []
                for b in range(chunks):
                    r = mm(left, src[rows(b), hs(h)])
                    blocks.append((r[:per] + r[per:]).astype(BF16))
                pooled = jnp.concatenate(blocks, axis=0)
                med_own[t, h] = pooled.T if t else pooled

    pl.semaphore_wait(barrier, others)
    loads[4].start()

    def q_copy(i):
        return remote(
            q_hbm.at[rows(i)], q_in.at[rows(i)], q_ss.at[i], q_rs.at[i],
            seq=jnp.maximum(pos - 1, 0),
        )

    def part(c):
        return pl.ds(pieces[c][0], pieces[c][1] - pieces[c][0])

    def oe_copy(c):
        return remote(
            oe_out.at[part(c)], oe_in.at[part(c)], oe_ss.at[c], oe_rs.at[c],
            seq=jnp.minimum(pos + 1, n_seq - 1),
        )

    def le_copy(i):
        return remote(
            le_out.at[i], le_in.at[i], le_ss.at[i], le_rs.at[i],
            seq=jnp.minimum(pos + 1, n_seq - 1),
        )

    def med_copy(slot, t):
        src = med_own if slot == 0 else med_in.at[0]
        return remote(
            src.at[t], med_in.at[slot, t], med_ss.at[slot, t], med_rs.at[slot, t],
            seq=jnp.minimum(pos + 2, n_seq - 1),
        )

    def c_copy(o, step):
        return remote(
            c_in.at[o], c_in.at[o], c_ss.at[step - 1, o], c_rs.at[o],
            seq=jnp.minimum(pos + step, n_seq - 1),
        )

    def c_send(o, act):
        for step in (2, 1):
            @pl.when(pos + step < n_seq)
            def _():
                act(c_copy(o, step))

    def cols(g, side):
        return pl.ds(pl.multiple_of((g * 2 + side) * width, width), width)

    def w_load(g):
        return pltpu.make_async_copy(w_hbm.at[:, cols(g, core)], w_v.at[0, g], w_sem.at[g])

    def w_copy(g):
        return remote(
            w_hbm.at[:, cols(g, 1 - core)], w_v.at[1, g], wx_ss.at[g], wx_rs.at[g], head=mate
        )

    def at_copy(c):
        return remote(attn.at[part(c)], attn_in.at[part(c)], at_ss.at[c], at_rs.at[c], head=mate)

    def far_copy(c, o, j):
        return remote(
            far_out.at[o - 1, j, part(c)], far_in.at[o - 1, j, part(c)],
            far_ss.at[c, o - 1, j], far_rs.at[c, o - 1, j],
            head=lax.rem(grp + o, groups) * 2 + core,
        )

    has_prev = pos >= 1
    has_next = pos < n_seq - 1

    @pl.when(has_prev)
    def _():
        for i in range(chunks):
            q_copy(i).start()

    @pl.when(pos + 2 < n_seq)
    def _():
        med_copy(0, 0).start()

    for g in range(groups):
        w_copy(g).start()
        w_load(g).start()
    c_row = lax.broadcasted_iota(jnp.int32, (2 * n_coarse, tok), 0)
    c_col = lax.broadcasted_iota(jnp.int32, (2 * n_coarse, tok), 1) // coarse

    @pl.loop(0, heads)
    def _(h):
        vt[h] = v_v[:, hs(h)].T
        totals = []
        for t, src in enumerate((k_v, v_v)):
            hi, lo = (
                jnp.concatenate([pat[1, n, t, pl.ds(h, 1), :]] * chunks, axis=1)
                for n in range(2)
            )
            left = jnp.where(c_col == c_row, hi, 0.0)
            left = jnp.where(c_col + n_coarse == c_row, lo, left).astype(BF16)
            r = mm(left, src[:, hs(h)])
            totals.append(r[:n_coarse] + r[n_coarse:])
        c_in[pos, h] = jnp.concatenate(totals, axis=0).astype(BF16)

    c_send(pos, lambda copy: copy.start())

    @pl.when(pos + 2 < n_seq)
    def _():
        med_copy(0, 1).start()

    loads[4].wait()

    def keep(i, h, o, m, total):
        o_loc[i, h] = o
        m_loc[i, pl.ds(h, 1), :] = m
        l_loc[i, pl.ds(h, 1), :] = total

    def softmax_parts(parts, m, total, o):
        for s, vals in parts:
            p = jnp.exp2((s - m) * scale)
            total = total + jnp.sum(p, axis=0, keepdims=True)
            o = o + mm(vals, p.astype(BF16))
        return total, o

    def peak(parts):
        return functools.reduce(
            jnp.maximum, [jnp.max(s, axis=0, keepdims=True) for s, _ in parts]
        )

    def own(i):
        first = i * wide

        @pl.loop(0, heads, unroll=2)
        def _(h):
            q = q_v[pl.ds(first, wide), hs(h)]
            parts = []
            if first:
                s = mm_nt(k_v[pl.ds(0, first), hs(h)], q)
                parts.append((s, vt[h, :, pl.ds(0, first)]))
            s = mm_nt(k_v[pl.ds(first, wide), hs(h)], q)
            key_at = lax.broadcasted_iota(jnp.int32, (wide, wide), 0)
            query_at = lax.broadcasted_iota(jnp.int32, (wide, wide), 1)
            s = jnp.where(key_at <= query_at, s, -jnp.inf)
            parts.append((s, vt[h, :, pl.ds(first, wide)]))
            m = peak(parts)
            total, o = softmax_parts(parts, m, 0.0, 0.0)
            keep(i, h, o, m, total)

    def edge(i):
        @pl.when(has_next)
        def _():
            @pl.loop(0, heads, unroll=2)
            def _(h):
                q = q_in[pl.ds(i * wide, wide), hs(h)]
                s = mm_nt(k_v[:, hs(h)], q)
                s2 = jnp.where(pos >= 2, mm_nt(med_in[0, 0, h], q), -jnp.inf)
                parts = [(s, vt[h]), (s2, med_in[0, 1, h])]
                m = peak(parts)
                total, o = softmax_parts(parts, m, 0.0, 0.0)
                oe_out[pl.ds(i * wide, wide), hs(h)] = (o / total).astype(BF16).T
                le_out[i, pl.ds(h, 1), :] = m * scale + jnp.log2(total)

            le_copy(i).start()

    def await_queries(i):
        @pl.when(has_next)
        def _():
            q_copy(2 * i).wait_recv()
            q_copy(2 * i + 1).wait_recv()

    def send_edge(low, high):
        @pl.when(has_next)
        def _():
            for c, (first, _) in enumerate(pieces):
                if low <= first < high:
                    oe_copy(c).start()

    def merge(i, h, parts):
        old = m_loc[i, pl.ds(h, 1), :]
        m = jnp.maximum(old, peak(parts))
        a = jnp.exp2((old - m) * scale)
        total, o = softmax_parts(parts, m, l_loc[i, pl.ds(h, 1), :] * a, o_loc[i, h] * a)
        keep(i, h, o, m, total)

    def near(i):
        @pl.loop(0, heads, unroll=2)
        def _(h):
            q = q_v[pl.ds(i * wide, wide), hs(h)]
            merge(i, h, [(mm_nt(med_in[0, 0, h], q), med_in[0, 1, h])])

    def far_keys():
        @pl.loop(0, n_seq)
        def _(o):
            @pl.when((o < pos) & (lax.rem(pos - o + n_seq * 2, 2) == 1))
            def _():
                c_copy(o, 1).wait_recv()

        @pl.loop(0, heads)
        def _(h):
            got = c_in[:, h].astype(F32)
            ck[h] = got[:, :n_coarse].reshape(n_seq * n_coarse, dim).astype(BF16)
            cvt[h] = got[:, n_coarse:].reshape(n_seq * n_coarse, dim).T.astype(BF16)

        @pl.when(pos >= 4)
        def _():
            med_copy(1, 0).wait_recv()
            med_copy(1, 1).wait_recv()

        @pl.when(has_prev)
        def _():
            distant(0)

    def distant(i):
        @pl.loop(0, heads, unroll=2)
        def _(h):
            q = q_v[pl.ds(i * wide, wide), hs(h)]
            s = mm_nt(med_in[1, 0, h], q)
            parts = [(jnp.where(pos >= 4, s, -jnp.inf), med_in[1, 1, h])]
            s = mm_nt(ck[h], q)
            owner = lax.broadcasted_iota(jnp.int32, s.shape, 0) // n_coarse
            parts.append((jnp.where(owner < pos, s, -jnp.inf), cvt[h]))
            merge(i, h, parts)

    def prepare(i):
        @pl.when(has_prev)
        def _():
            le_copy(i).wait_recv()

        mine = m_loc[i] * scale
        lse = le_in[i]
        top = jnp.maximum(mine, lse)
        a = jnp.exp2(mine - top)
        e = jnp.exp2(lse - top)
        inv = 1.0 / (l_loc[i] * a + e)
        a_loc[...] = a * inv
        e_col[pl.ds(i * wide, wide), :] = (e * inv).T

        @pl.loop(0, heads)
        def _(h):
            o_rows[pl.ds(i * wide, wide), hs(h)] = (o_loc[i, h] * a_loc[pl.ds(h, 1), :]).T

    def combine(c):
        @pl.when(has_prev)
        def _():
            oe_copy(c).wait_recv()

        for h in range(heads):
            at = slice(h * dim, (h + 1) * dim)
            o = o_rows[part(c), at] + oe_in[part(c), at].astype(F32) * e_col[part(c), h:h + 1]
            attn[part(c), at] = o.astype(BF16)
        at_copy(c).start()

    def mix(c):
        waited = False
        for o in list(range(1, groups)) + [0]:
            g = lax.rem(grp + o, groups)
            for j in range(tiles):
                at = pl.ds(j * tile, tile)
                acc[part(c), at] = mm(attn[part(c)], w_v[0, g, :, at])
            if not waited:
                at_copy(c).wait_recv()
                waited = True
            for j in range(tiles):
                at = pl.ds(j * tile, tile)
                value = acc[part(c), at] + mm(attn_in[part(c)], w_v[1, g, :, at])
                if o:
                    far_out[o - 1, j, part(c)] = value.astype(BF16)
                    far_copy(c, o, j).start()
                else:
                    acc[part(c), at] = value

    def final(c):
        for j in range(tiles):
            at = pl.ds(j * tile, tile)
            total = acc[part(c), at]
            for o in range(1, groups):
                far_copy(c, o, j).wait_recv()
                total = total + far_in[o - 1, j, part(c)].astype(F32)
            out_ref[part(c), at] = total.astype(BF16)

    def pass_on(t):
        @pl.when(pos >= 2)
        def _():
            med_copy(0, t).wait_recv()

            @pl.when(pos + 2 < n_seq)
            def _():
                med_copy(1, t).start()

    for i in range(halves):
        own(i)

    def relay(here):
        @pl.when(here)
        def _():
            @pl.loop(0, n_seq)
            def _(o):
                @pl.when((o < pos) & (lax.rem(pos - o + n_seq * 2, 2) == 0))
                def _():
                    c_copy(o, 1).wait_recv()
                    c_send(o, lambda copy: copy.start())

    relay(pos < 4)
    pass_on(0)
    relay((pos >= 4) & (pos < 6))
    pass_on(1)
    await_queries(0)
    edge(0)
    odd = lax.rem(pos, 2) == 1
    relay((pos >= 6) & jnp.logical_not(odd))

    @pl.when(jnp.logical_not(odd))
    def _():
        send_edge(0, wide)

    @pl.when(pos >= 2)
    def _():
        for i in range(halves):
            near(i)


    relay((pos >= 6) & odd)

    for i in range(1, halves):
        await_queries(i)
        if i == 1:
            @pl.when(odd)
            def _():
                send_edge(0, wide)

        edge(i)
        send_edge(i * wide, (i + 1) * wide)
    far_keys()
    for g in range(groups):
        w_load(g).wait()
        w_copy(g).wait_recv()

    for c, (first, _) in enumerate(pieces):
        if first % wide == 0:
            if first:
                @pl.when(has_prev)
                def _():
                    distant(first // wide)

            prepare(first // wide)
        combine(c)
        mix(c)
    for c in range(len(pieces)):
        final(c)

    @pl.when(has_prev)
    def _():
        for i in range(chunks):
            q_copy(i).wait_send()

    @pl.when(has_next)
    def _():
        for i in range(halves):
            le_copy(i).wait_send()
        for c in range(len(pieces)):
            oe_copy(c).wait_send()

    @pl.when(pos + 2 < n_seq)
    def _():
        med_copy(0, 0).wait_send()
        med_copy(0, 1).wait_send()

    @pl.when((pos >= 2) & (pos + 2 < n_seq))
    def _():
        med_copy(1, 0).wait_send()
        med_copy(1, 1).wait_send()

    @pl.loop(0, n_seq)
    def _(o):
        @pl.when((o <= pos) & (lax.rem(pos - o + n_seq * 2, 2) == 0))
        def _():
            c_send(o, lambda copy: copy.wait_send())

    for g in range(groups):
        w_copy(g).wait_send()
    for c in range(len(pieces)):
        at_copy(c).wait_send()
        for o in range(1, groups):
            for j in range(tiles):
                far_copy(c, o, j).wait_send()


def body(n_seq, n_head, queries, keys, values, med_weight, coarse_weight, out_weight):
    tok, feat = queries.shape
    heads, med = med_weight.shape[1:]
    dim = feat // heads
    row = dim
    chunks = tok // row
    wide = 2 * row
    halves = tok // wide
    pieces = len(row_pieces(tok, row))
    width = out_weight.shape[1] // n_head
    groups = n_head // 2
    far = max(groups - 1, 1)
    tile = math.gcd(width, 4 * dim)
    tiles = width // tile
    n_med = tok // med
    n_coarse = tok // coarse_weight.shape[2]
    dma = pltpu.SemaphoreType.DMA
    hbm = pl.BlockSpec(memory_space=pl.ANY)
    V = pltpu.VMEM
    scratch = [
        V((tok, feat), BF16), V((tok, feat), BF16), V((tok, feat), BF16),
        V((2, med, heads), F32), V(coarse_weight.shape, F32),
        V((2, 2, 2, heads, row), F32),
        V((2, groups, feat, width), BF16),
        V((heads, dim, tok), BF16),
        V((tok, feat), BF16),
        V((tok, feat), BF16),
        V((halves, heads, wide), F32),
        V((tok, feat), BF16),
        V((halves, heads, wide), F32),
        V((2, heads, n_med, dim), BF16),
        V((2, 2, heads, n_med, dim), BF16),
        V((n_seq, heads, 2 * n_coarse, dim), BF16),
        V((heads, n_seq * n_coarse, dim), BF16),
        V((heads, dim, n_seq * n_coarse), BF16),
        V((halves, heads, dim, wide), F32),
        V((halves, heads, wide), F32),
        V((halves, heads, wide), F32),
        V((heads, wide), F32),
        V((tok, heads), F32),
        V((tok, feat), F32),
        V((tok, feat), BF16),
        V((tok, feat), BF16),
        V((far, tiles, tok, tile), BF16),
        V((far, tiles, tok, tile), BF16),
        V((tok, width), F32),
        dma((5,)), dma((groups,)), dma((groups,)), dma((groups,)),
        dma((chunks,)), dma((chunks,)),
        dma((pieces,)), dma((pieces,)),
        dma((halves,)), dma((halves,)),
        dma((2, 2)), dma((2, 2)),
        dma((2, n_seq)), dma((n_seq,)),
        dma((pieces,)), dma((pieces,)),
        dma((pieces, far, tiles)), dma((pieces, far, tiles)),
    ]
    return pl.pallas_call(
        functools.partial(kernel, n_seq, n_head),
        out_shape=jax.ShapeDtypeStruct((tok, width), BF16),
        in_specs=[hbm] * 6,
        out_specs=pl.BlockSpec(memory_space=pltpu.VMEM),
        scratch_shapes=scratch,
        compiler_params=pltpu.CompilerParams(
            collective_id=0, has_side_effects=True, vmem_limit_bytes=48 * 1024 * 1024
        ),
    )(*(
        pltpu.with_memory_space_constraint(x, pltpu.HBM)
        for x in (
            queries, keys, values, med_weight.transpose(0, 2, 1), coarse_weight, out_weight
        )
    ))


def solution(mesh):
    placed = (
        P("seq", "head"),
        P("seq", "head"),
        P("seq", "head"),
        P(None, "head", None),
        P(None, "head", None),
        P("head", None),
    )
    return jax.shard_map(
        functools.partial(body, mesh.shape["seq"], mesh.shape["head"]),
        mesh=mesh, in_specs=placed, out_specs=P("seq", "head"), check_vma=False,
    )
```

```python
import functools
import math

import jax
import jax.numpy as jnp
from jax import lax
from jax.experimental import pallas as pl
from jax.experimental.pallas import tpu as pltpu
from jax.sharding import PartitionSpec as P

MESH = pl.DeviceIdType.MESH
F32 = jnp.float32
BF16 = jnp.bfloat16
LOG2E = math.log2(math.e)


def mm(a, b):
    return jnp.dot(a, b, preferred_element_type=F32)


def mm_nt(a, b):
    return lax.dot_general(a, b, (((1,), (1,)), ((), ())), preferred_element_type=F32)


def split(w):
    hi = w.astype(BF16)
    return hi, (w - hi.astype(F32)).astype(BF16)


def row_pieces(tok, row):
    cuts = list(range(0, tok, row)) + [tok - row // 2, tok]
    return list(zip(cuts[:-1], cuts[1:]))


def kernel(
    n_seq, n_head, q_hbm, k_hbm, v_hbm, wm_hbm, wc_hbm, w_hbm, out_ref,
    q_v, k_v, v_v, wm_v, wc_v, pat, w_v, vt, q_in, oe_out, le_out, oe_in, le_in,
    med_own, med_in, c_in, ck, cvt, o_loc, m_loc, l_loc, a_loc, e_col, o_rows,
    attn, attn_in, far_out, far_in, acc,
    ld_sem, w_sem, wx_ss, wx_rs, q_ss, q_rs, oe_ss, oe_rs, le_ss, le_rs, med_ss, med_rs,
    c_ss, c_rs, at_ss, at_rs, far_ss, far_rs,
):
    tok, feat = q_v.shape
    _, med, heads = wm_v.shape
    coarse = wc_v.shape[2]
    dim = feat // heads
    row = dim
    chunks = tok // row
    wide = 2 * row
    halves = tok // wide
    pieces = row_pieces(tok, row)
    n_med = tok // med
    n_coarse = tok // coarse
    width = out_ref.shape[1]
    tile = far_out.shape[3]
    tiles = width // tile
    scale = LOG2E / math.sqrt(dim)
    pos = lax.axis_index("seq")
    hd = lax.axis_index("head")
    groups = n_head // 2
    grp = hd // 2
    core = lax.rem(hd, 2)
    mate = grp * 2 + (1 - core)

    def remote(src, dst, ss, rs, **dev):
        return pltpu.make_async_remote_copy(
            src_ref=src, dst_ref=dst, send_sem=ss, recv_sem=rs,
            device_id=dev, device_id_type=MESH,
        )

    def hs(h):
        return pl.ds(pl.multiple_of(h * dim, dim), dim)

    loads = [
        pltpu.make_async_copy(s, d, ld_sem.at[n])
        for n, (s, d) in enumerate(
            ((wm_hbm, wm_v), (wc_hbm, wc_v), (k_hbm, k_v), (v_hbm, v_v), (q_hbm, q_v))
        )
    ]
    for ld in loads[:4]:
        ld.start()

    barrier = pltpu.get_barrier_semaphore()

    near_by = [(d, pos + d) for d in (-2, -1, 1, 2)]
    others = n_head - 1
    for d, to in near_by:
        there = to >= 0 if d < 0 else to < n_seq
        others = others + jnp.where(there, 1, 0)

        @pl.when(there)
        def _():
            pl.semaphore_signal(barrier, inc=1, device_id={"seq": to}, device_id_type=MESH)

    @pl.loop(1, n_head)
    def _(d):
        pl.semaphore_signal(
            barrier, inc=1, device_id={"head": lax.rem(hd + d, n_head)}, device_id_type=MESH
        )

    @pl.loop(0, n_seq)
    def _(o):
        @pl.when(o > pos)
        def _():
            c_in[o] = jnp.zeros(c_in.shape[1:], BF16)

    for slot in range(2):
        @pl.when(pos < 2 * slot + 2)
        def _():
            med_in[slot] = jnp.zeros(med_in.shape[1:], BF16)

    @pl.when(pos == 0)
    def _():
        oe_in[...] = jnp.zeros_like(oe_in)
        le_in[...] = jnp.full_like(le_in, -jnp.inf)

    loads[0].wait()
    loads[1].wait()
    for n, (src, size) in enumerate(((wm_v, med), (wc_v, coarse))):
        lane = lax.broadcasted_iota(jnp.int32, (size, row), 1)
        pick = lax.rem(lane, size) == lax.broadcasted_iota(jnp.int32, (size, row), 0)
        pick = jnp.where(pick, 1.0, 0.0).astype(BF16)
        for t in range(2):
            hi, lo = split(src[t] if n else src[t].T)
            pat[n, 0, t] = mm(hi, pick)
            pat[n, 1, t] = mm(lo, pick)

    def rows(i):
        return pl.ds(i * row, row)

    per = row // med
    sel = (lax.broadcasted_iota(jnp.int32, (per, row), 1) // med) == (
        lax.broadcasted_iota(jnp.int32, (per, row), 0)
    )
    loads[2].wait()
    loads[3].wait()

    @pl.when(pos + 2 < n_seq)
    def _():
        for t, src in enumerate((k_v, v_v)):
            @pl.loop(0, heads, unroll=2)
            def _(h):
                one = pl.ds(h, 1)
                left = jnp.concatenate(
                    [jnp.where(sel, pat[0, n, t, one, :], 0.0) for n in range(2)], axis=0
                ).astype(BF16)
                blocks = []
                for b in range(chunks):
                    r = mm(left, src[rows(b), hs(h)])
                    blocks.append((r[:per] + r[per:]).astype(BF16))
                pooled = jnp.concatenate(blocks, axis=0)
                med_own[t, h] = pooled.T if t else pooled

    pl.semaphore_wait(barrier, others)
    loads[4].start()

    def q_copy(i):
        return remote(
            q_hbm.at[rows(i)], q_in.at[rows(i)], q_ss.at[i], q_rs.at[i],
            seq=jnp.maximum(pos - 1, 0),
        )

    def part(c):
        return pl.ds(pieces[c][0], pieces[c][1] - pieces[c][0])

    def oe_copy(c):
        return remote(
            oe_out.at[part(c)], oe_in.at[part(c)], oe_ss.at[c], oe_rs.at[c],
            seq=jnp.minimum(pos + 1, n_seq - 1),
        )

    def le_copy(i):
        return remote(
            le_out.at[i], le_in.at[i], le_ss.at[i], le_rs.at[i],
            seq=jnp.minimum(pos + 1, n_seq - 1),
        )

    def med_copy(slot, t):
        src = med_own if slot == 0 else med_in.at[0]
        return remote(
            src.at[t], med_in.at[slot, t], med_ss.at[slot, t], med_rs.at[slot, t],
            seq=jnp.minimum(pos + 2, n_seq - 1),
        )

    def c_copy(o, step):
        return remote(
            c_in.at[o], c_in.at[o], c_ss.at[step - 1, o], c_rs.at[o],
            seq=jnp.minimum(pos + step, n_seq - 1),
        )

    def c_send(o, act):
        for step in (2, 1):
            @pl.when(pos + step < n_seq)
            def _():
                act(c_copy(o, step))

    def cols(g, side):
        return pl.ds(pl.multiple_of((g * 2 + side) * width, width), width)

    def w_load(g):
        return pltpu.make_async_copy(w_hbm.at[:, cols(g, core)], w_v.at[0, g], w_sem.at[g])

    def w_copy(g):
        return remote(
            w_hbm.at[:, cols(g, 1 - core)], w_v.at[1, g], wx_ss.at[g], wx_rs.at[g], head=mate
        )

    def at_copy(c):
        return remote(attn.at[part(c)], attn_in.at[part(c)], at_ss.at[c], at_rs.at[c], head=mate)

    def far_copy(c, o, j):
        return remote(
            far_out.at[o - 1, j, part(c)], far_in.at[o - 1, j, part(c)],
            far_ss.at[c, o - 1, j], far_rs.at[c, o - 1, j],
            head=lax.rem(grp + o, groups) * 2 + core,
        )

    has_prev = pos >= 1
    has_next = pos < n_seq - 1

    @pl.when(has_prev)
    def _():
        for i in range(chunks):
            q_copy(i).start()

    @pl.when(pos + 2 < n_seq)
    def _():
        med_copy(0, 0).start()

    for g in range(groups):
        w_copy(g).start()
        w_load(g).start()
    c_row = lax.broadcasted_iota(jnp.int32, (2 * n_coarse, tok), 0)
    c_col = lax.broadcasted_iota(jnp.int32, (2 * n_coarse, tok), 1) // coarse

    @pl.loop(0, heads)
    def _(h):
        vt[h] = v_v[:, hs(h)].T
        totals = []
        for t, src in enumerate((k_v, v_v)):
            hi, lo = (
                jnp.concatenate([pat[1, n, t, pl.ds(h, 1), :]] * chunks, axis=1)
                for n in range(2)
            )
            left = jnp.where(c_col == c_row, hi, 0.0)
            left = jnp.where(c_col + n_coarse == c_row, lo, left).astype(BF16)
            r = mm(left, src[:, hs(h)])
            totals.append(r[:n_coarse] + r[n_coarse:])
        c_in[pos, h] = jnp.concatenate(totals, axis=0).astype(BF16)

    c_send(pos, lambda copy: copy.start())

    @pl.when(pos + 2 < n_seq)
    def _():
        med_copy(0, 1).start()

    loads[4].wait()

    def keep(i, h, o, m, total):
        o_loc[i, h] = o
        m_loc[i, pl.ds(h, 1), :] = m
        l_loc[i, pl.ds(h, 1), :] = total

    def softmax_parts(parts, m, total, o):
        for s, vals in parts:
            p = jnp.exp2((s - m) * scale)
            total = total + jnp.sum(p, axis=0, keepdims=True)
            o = o + mm(vals, p.astype(BF16))
        return total, o

    def peak(parts):
        return functools.reduce(
            jnp.maximum, [jnp.max(s, axis=0, keepdims=True) for s, _ in parts]
        )

    def own(i):
        first = i * wide

        @pl.loop(0, heads, unroll=2)
        def _(h):
            q = q_v[pl.ds(first, wide), hs(h)]
            parts = []
            if first:
                s = mm_nt(k_v[pl.ds(0, first), hs(h)], q)
                parts.append((s, vt[h, :, pl.ds(0, first)]))
            s = mm_nt(k_v[pl.ds(first, wide), hs(h)], q)
            key_at = lax.broadcasted_iota(jnp.int32, (wide, wide), 0)
            query_at = lax.broadcasted_iota(jnp.int32, (wide, wide), 1)
            s = jnp.where(key_at <= query_at, s, -jnp.inf)
            parts.append((s, vt[h, :, pl.ds(first, wide)]))
            m = peak(parts)
            total, o = softmax_parts(parts, m, 0.0, 0.0)
            keep(i, h, o, m, total)

    def edge(i):
        @pl.when(has_next)
        def _():
            @pl.loop(0, heads, unroll=4)
            def _(h):
                q = q_in[pl.ds(i * wide, wide), hs(h)]
                s = mm_nt(k_v[:, hs(h)], q)
                s2 = jnp.where(pos >= 2, mm_nt(med_in[0, 0, h], q), -jnp.inf)
                parts = [(s, vt[h]), (s2, med_in[0, 1, h])]
                m = peak(parts)
                total, o = softmax_parts(parts, m, 0.0, 0.0)
                oe_out[pl.ds(i * wide, wide), hs(h)] = (o / total).astype(BF16).T
                le_out[i, pl.ds(h, 1), :] = m * scale + jnp.log2(total)

            le_copy(i).start()

    def await_queries(i):
        @pl.when(has_next)
        def _():
            q_copy(2 * i).wait_recv()
            q_copy(2 * i + 1).wait_recv()

    def send_edge(low, high):
        @pl.when(has_next)
        def _():
            for c, (first, _) in enumerate(pieces):
                if low <= first < high:
                    oe_copy(c).start()

    def merge(i, h, parts):
        old = m_loc[i, pl.ds(h, 1), :]
        m = jnp.maximum(old, peak(parts))
        a = jnp.exp2((old - m) * scale)
        total, o = softmax_parts(parts, m, l_loc[i, pl.ds(h, 1), :] * a, o_loc[i, h] * a)
        keep(i, h, o, m, total)

    def near(i):
        @pl.loop(0, heads, unroll=4)
        def _(h):
            q = q_v[pl.ds(i * wide, wide), hs(h)]
            merge(i, h, [(mm_nt(med_in[0, 0, h], q), med_in[0, 1, h])])

    def far_keys():
        @pl.loop(0, n_seq)
        def _(o):
            @pl.when((o < pos) & (lax.rem(pos - o + n_seq * 2, 2) == 1))
            def _():
                c_copy(o, 1).wait_recv()

        @pl.loop(0, heads)
        def _(h):
            got = c_in[:, h].astype(F32)
            ck[h] = got[:, :n_coarse].reshape(n_seq * n_coarse, dim).astype(BF16)
            cvt[h] = got[:, n_coarse:].reshape(n_seq * n_coarse, dim).T.astype(BF16)

        @pl.when(pos >= 4)
        def _():
            med_copy(1, 0).wait_recv()
            med_copy(1, 1).wait_recv()

        @pl.when(has_prev)
        def _():
            distant(0)

    def distant(i):
        @pl.loop(0, heads, unroll=4)
        def _(h):
            q = q_v[pl.ds(i * wide, wide), hs(h)]
            s = mm_nt(med_in[1, 0, h], q)
            parts = [(jnp.where(pos >= 4, s, -jnp.inf), med_in[1, 1, h])]
            s = mm_nt(ck[h], q)
            owner = lax.broadcasted_iota(jnp.int32, s.shape, 0) // n_coarse
            parts.append((jnp.where(owner < pos, s, -jnp.inf), cvt[h]))
            merge(i, h, parts)

    def prepare(i):
        @pl.when(has_prev)
        def _():
            le_copy(i).wait_recv()

        mine = m_loc[i] * scale
        lse = le_in[i]
        top = jnp.maximum(mine, lse)
        a = jnp.exp2(mine - top)
        e = jnp.exp2(lse - top)
        inv = 1.0 / (l_loc[i] * a + e)
        a_loc[...] = a * inv
        e_col[pl.ds(i * wide, wide), :] = (e * inv).T

        @pl.loop(0, heads)
        def _(h):
            o_rows[pl.ds(i * wide, wide), hs(h)] = (o_loc[i, h] * a_loc[pl.ds(h, 1), :]).T

    def combine(c):
        @pl.when(has_prev)
        def _():
            oe_copy(c).wait_recv()

        for h in range(heads):
            at = slice(h * dim, (h + 1) * dim)
            o = o_rows[part(c), at] + oe_in[part(c), at].astype(F32) * e_col[part(c), h:h + 1]
            attn[part(c), at] = o.astype(BF16)
        at_copy(c).start()

    def mix(c):
        for o in range(1, groups):
            g = lax.rem(grp + o, groups)
            for j in range(tiles):
                at = pl.ds(j * tile, tile)
                acc[part(c), at] = mm(attn[part(c)], w_v[0, g, :, at])
            if o == 1:
                at_copy(c).wait_recv()
            for j in range(tiles):
                at = pl.ds(j * tile, tile)
                value = acc[part(c), at] + mm(attn_in[part(c)], w_v[1, g, :, at])
                far_out[o - 1, j, part(c)] = value.astype(BF16)
                far_copy(c, o, j).start()

    def mix_own(i):
        span = pl.ds(i * wide, wide)
        for j in range(tiles):
            at = pl.ds(j * tile, tile)
            acc[span, at] = mm(attn[span], w_v[0, grp, :, at]) + mm(
                attn_in[span], w_v[1, grp, :, at]
            )

    def final(c):
        for j in range(tiles):
            at = pl.ds(j * tile, tile)
            total = acc[part(c), at]
            for o in range(1, groups):
                far_copy(c, o, j).wait_recv()
                total = total + far_in[o - 1, j, part(c)].astype(F32)
            out_ref[part(c), at] = total.astype(BF16)

    def pass_on(t):
        @pl.when(pos >= 2)
        def _():
            med_copy(0, t).wait_recv()

            @pl.when(pos + 2 < n_seq)
            def _():
                med_copy(1, t).start()

    for i in range(halves):
        own(i)

    def relay(here):
        @pl.when(here)
        def _():
            @pl.loop(0, n_seq)
            def _(o):
                @pl.when((o < pos) & (lax.rem(pos - o + n_seq * 2, 2) == 0))
                def _():
                    c_copy(o, 1).wait_recv()
                    c_send(o, lambda copy: copy.start())

    relay(pos < 4)
    pass_on(0)
    relay((pos >= 4) & (pos < 6))
    pass_on(1)
    await_queries(0)
    edge(0)
    odd = lax.rem(pos, 2) == 1
    relay((pos >= 6) & jnp.logical_not(odd))

    @pl.when(jnp.logical_not(odd))
    def _():
        send_edge(0, wide)

    @pl.when(pos >= 2)
    def _():
        for i in range(halves):
            near(i)


    relay((pos >= 6) & odd)

    for i in range(1, halves):
        @pl.when(odd)
        def _():
            await_queries(i)
            if i == 1:
                send_edge(0, wide)

        if i == 1:
            far_keys()

        @pl.when(jnp.logical_not(odd))
        def _():
            await_queries(i)

        edge(i)
        send_edge(i * wide, (i + 1) * wide)
    for g in range(groups):
        w_load(g).wait()
        w_copy(g).wait_recv()

    for c, (first, _) in enumerate(pieces):
        if first % wide == 0:
            if first:
                @pl.when(has_prev)
                def _():
                    distant(first // wide)

            prepare(first // wide)
        combine(c)
        mix(c)
    if groups == 1:
        for c in range(len(pieces)):
            at_copy(c).wait_recv()
    for i in range(halves):
        mix_own(i)
    for c in range(len(pieces)):
        final(c)

    @pl.when(has_prev)
    def _():
        for i in range(chunks):
            q_copy(i).wait_send()

    @pl.when(has_next)
    def _():
        for i in range(halves):
            le_copy(i).wait_send()
        for c in range(len(pieces)):
            oe_copy(c).wait_send()

    @pl.when(pos + 2 < n_seq)
    def _():
        med_copy(0, 0).wait_send()
        med_copy(0, 1).wait_send()

    @pl.when((pos >= 2) & (pos + 2 < n_seq))
    def _():
        med_copy(1, 0).wait_send()
        med_copy(1, 1).wait_send()

    @pl.loop(0, n_seq)
    def _(o):
        @pl.when((o <= pos) & (lax.rem(pos - o + n_seq * 2, 2) == 0))
        def _():
            c_send(o, lambda copy: copy.wait_send())

    for g in range(groups):
        w_copy(g).wait_send()
    for c in range(len(pieces)):
        at_copy(c).wait_send()
        for o in range(1, groups):
            for j in range(tiles):
                far_copy(c, o, j).wait_send()


def body(n_seq, n_head, queries, keys, values, med_weight, coarse_weight, out_weight):
    tok, feat = queries.shape
    heads, med = med_weight.shape[1:]
    dim = feat // heads
    row = dim
    chunks = tok // row
    wide = 2 * row
    halves = tok // wide
    pieces = len(row_pieces(tok, row))
    width = out_weight.shape[1] // n_head
    groups = n_head // 2
    far = max(groups - 1, 1)
    tile = math.gcd(width, 4 * dim)
    tiles = width // tile
    n_med = tok // med
    n_coarse = tok // coarse_weight.shape[2]
    dma = pltpu.SemaphoreType.DMA
    hbm = pl.BlockSpec(memory_space=pl.ANY)
    V = pltpu.VMEM
    scratch = [
        V((tok, feat), BF16), V((tok, feat), BF16), V((tok, feat), BF16),
        V((2, med, heads), F32), V(coarse_weight.shape, F32),
        V((2, 2, 2, heads, row), F32),
        V((2, groups, feat, width), BF16),
        V((heads, dim, tok), BF16),
        V((tok, feat), BF16),
        V((tok, feat), BF16),
        V((halves, heads, wide), F32),
        V((tok, feat), BF16),
        V((halves, heads, wide), F32),
        V((2, heads, n_med, dim), BF16),
        V((2, 2, heads, n_med, dim), BF16),
        V((n_seq, heads, 2 * n_coarse, dim), BF16),
        V((heads, n_seq * n_coarse, dim), BF16),
        V((heads, dim, n_seq * n_coarse), BF16),
        V((halves, heads, dim, wide), F32),
        V((halves, heads, wide), F32),
        V((halves, heads, wide), F32),
        V((heads, wide), F32),
        V((tok, heads), F32),
        V((tok, feat), F32),
        V((tok, feat), BF16),
        V((tok, feat), BF16),
        V((far, tiles, tok, tile), BF16),
        V((far, tiles, tok, tile), BF16),
        V((tok, width), F32),
        dma((5,)), dma((groups,)), dma((groups,)), dma((groups,)),
        dma((chunks,)), dma((chunks,)),
        dma((pieces,)), dma((pieces,)),
        dma((halves,)), dma((halves,)),
        dma((2, 2)), dma((2, 2)),
        dma((2, n_seq)), dma((n_seq,)),
        dma((pieces,)), dma((pieces,)),
        dma((pieces, far, tiles)), dma((pieces, far, tiles)),
    ]
    return pl.pallas_call(
        functools.partial(kernel, n_seq, n_head),
        out_shape=jax.ShapeDtypeStruct((tok, width), BF16),
        in_specs=[hbm] * 6,
        out_specs=pl.BlockSpec(memory_space=pltpu.VMEM),
        scratch_shapes=scratch,
        compiler_params=pltpu.CompilerParams(
            collective_id=0, has_side_effects=True, vmem_limit_bytes=48 * 1024 * 1024
        ),
    )(*(
        pltpu.with_memory_space_constraint(x, pltpu.HBM)
        for x in (
            queries, keys, values, med_weight.transpose(0, 2, 1), coarse_weight, out_weight
        )
    ))


def solution(mesh):
    placed = (
        P("seq", "head"),
        P("seq", "head"),
        P("seq", "head"),
        P(None, "head", None),
        P(None, "head", None),
        P("head", None),
    )
    return jax.shard_map(
        functools.partial(body, mesh.shape["seq"], mesh.shape["head"]),
        mesh=mesh, in_specs=placed, out_specs=P("seq", "head"), check_vma=False,
    )
```
